32 devices in a mesh: ka: 4 (over y, core), op: 4 (over z), row: 2 (over x).
Axes of the slice: x: 2, y: 2, z: 4, core: 2. Of those that a mesh axis runs over, the one named last changes fastest.
Arguments:
- kgrid: int32 [3, 256], P(None, ('ka', 'op', 'row')), may hold values from 0 to 63
- rvec: int32 [3, 256], replicated, may hold values from -8 to 8
- degen: int32 [256], replicated, may hold values from 1 to 4
- operators: bfloat16 [4, 256, 12800], P('op', ('ka', 'row')), may hold values from -1 to 1
- vectors: bfloat16 [256, 12800], P(('ka', 'op', 'row')), may hold values from -0.5 to 0.5
Outputs:
- density: float32 [3, 256], P(None, ('ka', 'op', 'row'))
- magnetization: float32 [3], replicated
The draws below stay inside these ranges and needn't reach their ends.
All inputs are finite; a program needn't handle non-finite values.
Results may differ from the reference program's by a relative error of at most 0.012.
Values may be sent and summed in bfloat16 or wider, within the bound.
No kernel may reach another device: no remote copies, remote signals or barrier semaphores. Data moves between devices by JAX's collectives and lax.ppermute only.
A program may use at most 64 MiB of HBM per device.

```python
import math
import jax
import jax.numpy as jnp
from jax import lax

W = 80
GRID = 64
NR = 256
KPT = 8
KPOINTS = 256


def draw_operators(key, part):
    base = jax.random.normal(jax.random.fold_in(key, 11), (4, NR, 2 * W * W), jnp.float32)
    spread = 1.5 / math.sqrt(NR)
    return jnp.clip(base * spread, -1.0, 1.0).astype(jnp.bfloat16)


def place_ends(entries, stream_key, smallest, top_value):
    index_at = [jax.random.randint(jax.random.fold_in(stream_key, axis), (), 0, length) for axis, length in enumerate(entries.shape)]
    main_axis = entries.shape.index(max(entries.shape))
    neighbour = index_at[:main_axis] + [(index_at[main_axis] + 1) % entries.shape[main_axis]] + index_at[main_axis + 1:]
    return entries.at[tuple(index_at)].set(smallest).at[tuple(neighbour)].set(top_value)


def block_scale(key, dims, cuts, smallest, largest):
    loudness = 1.0
    for dim, parts in cuts:
        draws = jax.random.uniform(jax.random.fold_in(jax.random.fold_in(key, 6), dim), (parts,), jnp.float32, smallest / len(cuts), largest / len(cuts))
        loudness = loudness * jnp.repeat(jnp.exp(draws), dims[dim] // parts).reshape((-1,) + (1,) * (len(dims) - 1 - dim))
    return loudness


def scatter_about(own_key, extent, deviation, most, split=(), kind=jnp.bfloat16):
    result = deviation * jax.random.normal(own_key, extent, jnp.float32)
    if split:
        result = result * block_scale(own_key, extent, split, -0.22, 0.18)
    return jnp.clip(result, -most, most).astype(kind)


def setup_inputs(seed: int = 0) -> dict:
    seeds = jax.random.split(jax.random.key(seed), 6)
    kgrid = place_ends(jax.random.randint(seeds[0], (3, KPOINTS), 0, GRID), jax.random.fold_in(seeds[0], 1), 0, GRID - 1).astype(jnp.int32)
    rvec = place_ends(jax.random.randint(seeds[1], (3, NR), -8, 9), jax.random.fold_in(seeds[1], 1), -8, 8).astype(jnp.int32)
    degen = place_ends(jax.random.randint(seeds[2], (NR,), 1, 5), jax.random.fold_in(seeds[2], 1), 1, 4).astype(jnp.int32)
    operators = draw_operators(jax.random.fold_in(seeds[5], 71), 0)
    vectors = scatter_about(seeds[4], (KPOINTS, 2 * W * W), (2 * W) ** -0.5, 0.5, ((0, 32),))
    return dict(kgrid=kgrid, rvec=rvec, degen=degen, operators=operators, vectors=vectors)


SMEARING = 0.5


def phase_pair(points, lattice, weights):
    winding = points[0][:, None] * lattice[0][None, :] + points[1][:, None] * lattice[1][None, :] + points[2][:, None] * lattice[2][None, :]
    winding = jnp.mod(winding, GRID)
    angle = (2.0 * math.pi / GRID) * winding.astype(jnp.float32)
    inverse = 1.0 / weights.astype(jnp.float32)
    cosine = (jnp.cos(angle) * inverse[None, :]).astype(jnp.bfloat16)
    sine = (jnp.sin(angle) * inverse[None, :]).astype(jnp.bfloat16)
    return cosine, sine


def transform(points, matrices, rvec, degen):
    cosine, sine = phase_pair(points, rvec, degen)
    cosine = cosine.astype(jnp.float32)
    sine = sine.astype(jnp.float32)
    half = matrices.shape[2] // 2
    real_in = matrices[:, :, :half].astype(jnp.float32)
    imag_in = matrices[:, :, half:].astype(jnp.float32)

    def mix(table, block):
        return jnp.einsum("kr,orx->okx", table, block)

    real_k = (mix(cosine, real_in) - mix(sine, imag_in)).astype(jnp.bfloat16)
    imag_k = (mix(cosine, imag_in) + mix(sine, real_in)).astype(jnp.bfloat16)
    return real_k, imag_k


def rotate_all(real_k, imag_k, vec_real, vec_imag):
    op_real = real_k.astype(jnp.float32)
    op_imag = imag_k.astype(jnp.float32)
    vr = vec_real.astype(jnp.float32)
    vi = vec_imag.astype(jnp.float32)
    prod_real = (jnp.einsum("okij,kjn->okin", op_real, vr) - jnp.einsum("okij,kjn->okin", op_imag, vi)).astype(jnp.bfloat16).astype(jnp.float32)
    prod_imag = (jnp.einsum("okij,kjn->okin", op_real, vi) + jnp.einsum("okij,kjn->okin", op_imag, vr)).astype(jnp.bfloat16).astype(jnp.float32)
    rot_real = (jnp.einsum("kin,okim->oknm", vr, prod_real) + jnp.einsum("kin,okim->oknm", vi, prod_imag)).astype(jnp.bfloat16)
    rot_imag = (jnp.einsum("kin,okim->oknm", vr, prod_imag) - jnp.einsum("kin,okim->oknm", vi, prod_real)).astype(jnp.bfloat16)
    return rot_real, rot_imag


def density_terms(rot_real, rot_imag):
    ham_real = rot_real[0].astype(jnp.float32)
    ham_imag = rot_imag[0].astype(jnp.float32)
    conn_real = rot_real[1:].astype(jnp.float32)
    conn_imag = rot_imag[1:].astype(jnp.float32)
    levels = jnp.diagonal(ham_real, axis1=1, axis2=2)
    filled = jax.nn.sigmoid(-levels / SMEARING)
    vacant = 1.0 - filled
    prod_real = jnp.einsum("knm,bkml->bknl", ham_real, conn_real) - jnp.einsum("knm,bkml->bknl", ham_imag, conn_imag)
    prod_imag = jnp.einsum("knm,bkml->bknl", ham_real, conn_imag) + jnp.einsum("knm,bkml->bknl", ham_imag, conn_real)
    weight = filled[None, :, :, None] * vacant[None, :, None, :]
    left_real = conn_real * weight
    left_imag = conn_imag * weight
    traces = jnp.einsum("aknm,bkmn->abk", left_real, prod_imag, precision=lax.Precision.HIGHEST) + jnp.einsum("aknm,bkmn->abk", left_imag, prod_real, precision=lax.Precision.HIGHEST)
    density = jnp.stack([traces[1, 2] - traces[2, 1], traces[2, 0] - traces[0, 2], traces[0, 1] - traces[1, 0]])
    return density / W


def reference(kgrid, rvec, degen, operators, vectors):
    blocks_count = KPOINTS // KPT
    blocks = kgrid.reshape(3, blocks_count, KPT).transpose(1, 0, 2)
    vector_blocks = vectors.reshape(blocks_count, KPT, 2, W, W)

    def block_density(bundle):
        points, vec = bundle
        real_k, imag_k = transform(points, operators, rvec, degen)
        real_k = real_k.reshape(4, KPT, W, W)
        imag_k = imag_k.reshape(4, KPT, W, W)
        rot_real, rot_imag = rotate_all(real_k, imag_k, vec[:, 0], vec[:, 1])
        return density_terms(rot_real, rot_imag)

    pieces = lax.map(block_density, (blocks, vector_blocks))
    density = pieces.transpose(1, 0, 2).reshape(3, KPOINTS)
    magnetization = jnp.sum(density, axis=1) / KPOINTS
    return density, magnetization
```

```python
import functools
import math

import jax
import jax.numpy as jnp
from jax import lax
from jax.experimental import pallas as pl
from jax.experimental.pallas import tpu as pltpu
from jax.sharding import Mesh
from jax.sharding import PartitionSpec as P


GRID = 64
SMEARING = 0.5
CORES = 2
LANES = 128
SUBLANES = 8
TOP = float(2**19)
TINY = 1e-30
ALL = ("y", "core", "op", "row")
BF16 = jnp.bfloat16
F32 = jnp.float32
NT = (((1,), (1,)), ((), ()))
NN = (((1,), (0,)), ((), ()))
TN = (((0,), (0,)), ((), ()))


def dot(left, right, dims):
    return lax.dot_general(left, right, dims, preferred_element_type=F32)


def vmem(count):
    return [pl.BlockSpec(memory_space=pltpu.VMEM)] * count


def call(kernel, outs, operands, flops, scratch=()):
    return pl.pallas_call(
        kernel,
        out_shape=outs,
        in_specs=vmem(len(operands)),
        out_specs=vmem(len(outs)),
        scratch_shapes=list(scratch),
        cost_estimate=pl.CostEstimate(
            flops=flops, bytes_accessed=10**5, transcendentals=0
        ),
        compiler_params=pltpu.CompilerParams(vmem_limit_bytes=16 * 2**20),
    )(*operands)


def block_sources(sizes, y, c, x):
    ny, _, _, nx = sizes
    sources = [(y, c, x)]
    for s in range(1, nx):
        back_x = lax.rem(x - s + nx, nx)
        if nx == ny:
            from_y = jnp.where(c == 0, y, lax.rem(y - s + ny, ny))
            from_x = jnp.where(c == 0, back_x, x)
        else:
            from_y, from_x = y, back_x
        sources += [(from_y, c, from_x), (from_y, 1 - c, from_x)]
    return sources + [(y, 1 - c, x)]


def flat_pairs(sizes, move):
    ny, nc, nz, nx = sizes

    def flat(y, c, z, x):
        return ((y * nc + c) * nz + z) * nx + x

    return [
        (flat(y, c, z, x), flat(*move(y, c, z, x)))
        for y in range(ny)
        for c in range(nc)
        for z in range(nz)
        for x in range(nx)
    ]


SINE = [
    (-1) ** n * math.pi ** (2 * n + 1) / math.factorial(2 * n + 1) for n in range(8)
]


def cut_kernel(quarter, cells, mine, theirs):
    core = lax.axis_index("core")
    depth = cells.shape[1]
    for out, which in ((mine, core), (theirs, 1 - core)):
        for ri in range(2):
            start = pl.multiple_of((2 * ri + which) * quarter, LANES)
            out[ri * depth : (ri + 1) * depth, :] = cells[0, :, pl.ds(start, quarter)]


def points_kernel(sizes, own, kgrid, cells, out):
    del cells
    row = lax.broadcasted_iota(jnp.int32, out.shape, 0)
    lane = lax.broadcasted_iota(jnp.int32, out.shape, 1)
    wide = jnp.concatenate(
        [kgrid[...], kgrid[...], jnp.zeros((3, LANES - 2 * own), jnp.int32)], axis=1
    )
    value = jnp.zeros(out.shape, jnp.int32)
    for n in range(3):
        value = jnp.where(row == n, wide[n : n + 1], value)
    imag = jnp.logical_and(lane >= own, lane < 2 * own)
    value = jnp.where(row == 3, jnp.where(imag, -(GRID // 4), 0), value)
    value = jnp.where(jnp.logical_and(row == 4, lane < 2 * own), 1, value)
    at = (lax.axis_index("op") * sizes[1] + lax.axis_index("core")) * 2 * own
    out[...] = pltpu.roll(value, at, 1)


def join_kernel(*refs):
    value = refs[0][...]
    for ref in refs[1:-1]:
        value = value + ref[...]
    refs[-1][...] = value


def ordered(points, sizes, order, own):
    _, nc, nz, _ = sizes
    z, c = lax.axis_index("op"), lax.axis_index("core")
    lane = lax.broadcasted_iota(jnp.int32, points.shape, 1)
    value = points
    for n, s in enumerate(order):
        for dc in range(nc):
            source = lax.rem(z + s, nz) * nc + lax.rem(c + dc, nc)
            target = n * nc + dc
            moved = pltpu.roll(points, lax.rem(target - source + nz * nc, nz * nc) * 2 * own, 1)
            inside = jnp.logical_and(lane >= target * 2 * own, lane < (target + 1) * 2 * own)
            value = jnp.where(inside, moved, value)
    return value


def table_kernel(sizes, order, own, depth, sets, rvec, degen, *refs):
    _, nc, _, nx = sizes
    y, c, x = (lax.axis_index(name) for name in ("y", "core", "row"))
    terms = refs[sets].shape[1]
    sources = block_sources(sizes, y, c, x)
    row = lax.broadcasted_iota(jnp.int32, (SUBLANES, degen.shape[1]), 0)
    plain = jnp.zeros(row.shape, jnp.int32)
    for n in range(3):
        plain = jnp.where(row == n, rvec[n : n + 1, :], plain)
    plain = jnp.where(row == 3, 1, plain)
    plain = jnp.where(row == 5, degen[...], plain)
    total = degen.shape[1]
    width = max(terms, total)
    if total < width:
        plain = jnp.concatenate(
            [plain, jnp.zeros((SUBLANES, width - total), jnp.int32)], axis=1
        )
    row = lax.broadcasted_iota(jnp.int32, (SUBLANES, width), 0)
    lane = lax.broadcasted_iota(jnp.int32, (SUBLANES, width), 1)
    lattice = jnp.ones((SUBLANES, width), jnp.int32)
    for n, (sy, sc, sx) in enumerate(sources):
        base = ((sy * nc + sc) * nx + sx) * depth
        for ri in range(2):
            target = (2 * n + ri) * depth
            moved = pltpu.roll(plain, lax.rem(target - base + width, width), 1)
            moved = jnp.where(row == 4, ri * (GRID // 4), moved)
            inside = jnp.logical_and(lane >= target, lane < target + depth)
            lattice = jnp.where(inside, moved, lattice)
    lattice = lattice[:, :terms]
    scale = 1.0 / lattice[5:6].astype(F32)
    lattice = lattice.astype(BF16)
    for points, out in zip(refs[:sets], refs[sets:]):
        chosen = ordered(points[...], sizes, order, own).astype(BF16)
        winding = dot(chosen, lattice, TN).astype(jnp.int32)
        turn = jnp.bitwise_and(winding + GRID // 2, GRID - 1) - GRID // 2
        u = 0.5 - jnp.abs(turn).astype(F32) * (2.0 / GRID)
        square = u * u
        value = SINE[7]
        for n in range(6, -1, -1):
            value = value * square + SINE[n]
        out[...] = (value * u * scale).astype(BF16)


def fold_kernel(blocks, tables, coded, skip, *refs):
    stacked = jnp.concatenate([ref[...] for ref in refs[:blocks]], axis=0)
    outs = refs[blocks + tables :]
    each = len(outs) // tables
    quarter = stacked.shape[1]
    for t in range(tables):
        rows = outs[t * each].shape[0]
        rows = rows * 4 // 5 if coded else rows
        chosen = refs[blocks + t][skip * rows : (skip + each) * rows, :]
        product = dot(chosen, stacked, NN)
        for n in range(each):
            out = outs[t * each + n]
            value = product[n * rows : (n + 1) * rows]
            if not coded:
                out[...] = value
                continue
            step = rows // 4
            most = jnp.max(jnp.abs(value), axis=1, keepdims=True)
            power = jnp.ceil(jnp.log2(jnp.maximum(most, TINY)))
            value = jnp.round(value * (TOP * jnp.exp2(-power)))
            value = jnp.clip(value, -TOP, TOP - 1.0).astype(jnp.int32)
            out[:rows, :quarter] = jnp.right_shift(value, 4).astype(jnp.int16)
            low = jnp.bitwise_and(value, 15)
            packed = low[:step]
            for g in range(1, 4):
                packed = packed + jnp.left_shift(low[g * step : (g + 1) * step], 4 * g)
            packed = jnp.where(packed > 32767, packed - 65536, packed)
            out[rows:, :quarter] = packed.astype(jnp.int16)
            power = jnp.broadcast_to(power, (rows, LANES)).astype(jnp.int32)
            out[:rows, quarter:] = power.astype(jnp.int16)
            out[rows:, quarter:] = jnp.zeros((step, LANES), jnp.int16)


def padded(value, rows, lanes):
    if value.shape[1] < lanes:
        fill = jnp.zeros((value.shape[0], lanes - value.shape[1]), value.dtype)
        value = jnp.concatenate([value, fill], axis=1)
    if value.shape[0] < rows:
        fill = jnp.zeros((rows - value.shape[0], value.shape[1]), value.dtype)
        value = jnp.concatenate([value, fill], axis=0)
    return value


def add_kernel(*refs):
    value = refs[0][...]
    rows, quarter = value.shape
    step = rows // 4
    sources = [ref for ref in refs[1:] if ref.shape[0] == rows + step]
    outs = refs[1 + len(sources) :]
    for ref in sources:
        packed = ref[rows:, :quarter].astype(jnp.int32)
        low = [jnp.bitwise_and(jnp.right_shift(packed, 4 * g), 15) for g in range(4)]
        high = ref[:rows, :quarter].astype(jnp.int32)
        term = jnp.left_shift(high, 4) + jnp.concatenate(low, axis=0)
        power = ref[:rows, quarter:].astype(jnp.int32).astype(F32)[:, :1]
        value = value + term.astype(F32) * (jnp.exp2(power) / TOP)
    value = value.astype(BF16)
    at = 0
    for out in outs:
        out[...] = value[at : at + out.shape[0]]
        at += out.shape[0]


def split_kernel(both, out):
    out[...] = both[out.shape[0] :]


def spread(source, start, width, count, store):
    for i in range(count):
        piece = source[:, start + i * width : start + (i + 1) * width]
        store(i, padded(piece, piece.shape[0], -(-width // LANES) * LANES))


def BANDS_SCRATCH(own, width, lanes):
    return [pltpu.VMEM((2 * width * own, lanes), F32)]


def TURN_SCRATCH(own, width, lanes):
    return [pltpu.VMEM((2 * width * own, lanes), F32)]


def bands_kernel(own, width, lanes, vectors, first, second, third, rows):
    for ri in range(2):
        source = vectors[:, ri * width * width : (ri + 1) * width * width].astype(F32)

        def store(i, piece, ri=ri):
            rows[pl.ds((ri * width + i) * own, own), :] = piece

        spread(source, 0, width, width, store)
    for k in range(own):
        real = padded(rows[pl.ds(k, width, stride=own), :], lanes, lanes)
        imag = padded(rows[pl.ds(width * own + k, width, stride=own), :], lanes, lanes)
        real_t = real.T[:width].astype(BF16)
        imag_t = imag.T[:width].astype(BF16)
        real = real.astype(BF16)
        imag = imag.astype(BF16)
        first[k, :width, :lanes] = real_t
        first[k, :width, lanes:] = -imag_t
        first[k, width:, :lanes] = imag_t
        first[k, width:, lanes:] = real_t
        second[k, :width, :lanes] = real_t
        second[k, :width, lanes:] = imag_t
        second[k, width:, :lanes] = -imag_t
        second[k, width:, lanes:] = real_t
        third[k, :lanes, :lanes] = real
        third[k, :lanes, lanes:] = -imag
        third[k, lanes:, :lanes] = imag
        third[k, lanes:, lanes:] = real


def turn_kernel(own, width, lanes, same, cross, first, second, third, rot, turned, rows):
    core = lax.axis_index("core")
    half = width // 2
    for ref, which in ((same, core), (cross, 1 - core)):
        for ri in range(2):

            def store(i, piece, ri=ri, which=which):
                at = pl.multiple_of((ri * width + which * half + i) * own, own)
                rows[pl.ds(at, own), :] = piece

            source = ref[ri * own : (ri + 1) * own, :].astype(F32)
            spread(source, 0, width, half, store)
    prods = []
    for k in range(own):
        parts = [
            padded(
                rows[pl.ds(ri * width * own + k, width, stride=own), :].astype(BF16), lanes, lanes
            )
            for ri in range(2)
        ]
        both = jnp.concatenate(parts, axis=1)
        mixed = dot(first[k], both, NT).astype(BF16)
        prods.append(jnp.concatenate([mixed[:width], mixed[width:]], axis=1))
    for k in range(own):
        rot[k] = dot(second[k], padded(prods[k], lanes, 2 * lanes), NT).astype(BF16)
        turned[k] = dot(prods[k], third[k], NN).astype(BF16)


def trace_kernel(nops, own, width, lanes, *refs):
    rots = refs[:nops]
    turns = refs[nops : 2 * nops]
    density_ref, total_ref, prod_ref, acc_ref = refs[2 * nops :]
    row = lax.broadcasted_iota(jnp.int32, (width, lanes), 0)
    col = lax.broadcasted_iota(jnp.int32, (width, lanes), 1)
    on_diagonal = row == col

    def multiply(k, order):
        ham = turns[order[0]][k]
        ham = jnp.concatenate(
            [
                padded(ham, lanes, 2 * lanes),
                padded(jnp.concatenate([-ham[:, lanes:], ham[:, :lanes]], axis=1), lanes, 2 * lanes),
            ],
            axis=0,
        )
        connections = jnp.concatenate([turns[n][k] for n in order[1:]], axis=0)
        prod_ref[k] = dot(connections, ham, NN)

    def one(k, order):
        levels = jnp.where(on_diagonal, rots[order[0]][k, :width].astype(F32), 0.0)
        filled = 1.0 / (1.0 + jnp.exp(jnp.sum(levels, axis=1, keepdims=True) / SMEARING))
        vacant = 1.0 - 1.0 / (1.0 + jnp.exp(jnp.sum(levels, axis=0, keepdims=True) / SMEARING))
        weight = filled * vacant
        left_re = [rots[n][k, :width].astype(F32) for n in order[1:]]
        left_im = [rots[n][k, width:].astype(F32) for n in order[1:]]
        prod_re = [prod_ref[k, n * width : (n + 1) * width, :lanes] for n in range(nops - 1)]
        prod_im = [prod_ref[k, n * width : (n + 1) * width, lanes:] for n in range(nops - 1)]
        for c, (a, b) in enumerate(((1, 2), (2, 0), (0, 1))):
            terms = weight * (
                left_re[a] * prod_im[b]
                + left_im[a] * prod_re[b]
                - left_re[b] * prod_im[a]
                - left_im[b] * prod_re[a]
            )
            acc_ref[c, k : k + 1, :] = jnp.sum(terms, axis=0, keepdims=True)

    for depth in range(nops):
        order = [(depth - name) % nops for name in range(nops)]

        @pl.when(lax.axis_index("op") == depth)
        def _(order=order):
            for k in range(own):
                multiply(k, order)
            for k in range(own):
                one(k, order)

    small_row = lax.broadcasted_iota(jnp.int32, (own, own), 0)
    small_col = lax.broadcasted_iota(jnp.int32, (own, own), 1)
    lane = lax.broadcasted_iota(jnp.int32, total_ref.shape, 1)
    total = jnp.zeros(total_ref.shape, F32)
    for c in range(3):
        each = jnp.sum(acc_ref[c], axis=1, keepdims=True) / width
        line = jnp.sum(jnp.where(small_row == small_col, each, 0.0), axis=0, keepdims=True)
        density_ref[c : c + 1, :] = line
        summed = jnp.sum(line, axis=1, keepdims=True)
        total = jnp.where(lane == c, summed, total)
    total_ref[...] = total / (own * total_ref.shape[0])


def TRACE_SCRATCH(nops, own, width, lanes):
    return [
        pltpu.VMEM((own, (nops - 1) * width, 2 * lanes), F32),
        pltpu.VMEM((3, own, lanes), F32),
    ]


def per_device(sizes, *args):
    return on_device(sizes, *args)


def on_device(sizes, kgrid, rvec, degen, operators, vectors):
    ny, nc, nz, nx = sizes
    count = ny * nc * nz * nx
    own = kgrid.shape[1]
    depth = operators.shape[1]
    quarter = operators.shape[2] // 4
    width = math.isqrt(vectors.shape[1] // 2)
    lanes = -(-width // LANES) * LANES
    mixed = nx == ny

    def along_row(core):
        return core == 0 or not mixed

    def gather_to(y, c, z, x, s):
        return (y, c, z, (x + s) % nx) if along_row(c) else ((y + s) % ny, c, z, x)

    def reduce_to(y, c, z, x, s):
        return ((y + s) % ny, c, z, x) if along_row(c) else (y, c, z, (x + s) % nx)

    def send(value, move):
        return lax.ppermute(value, ALL, flat_pairs(sizes, move))

    order = sorted(range(nz), key=lambda s: -min(s, nz - s))
    int_row = [jax.ShapeDtypeStruct((SUBLANES, LANES), jnp.int32)]

    def join(*pieces):
        return call(join_kernel, int_row, list(pieces), 10**3)[0]

    points = call(
        functools.partial(points_kernel, sizes, own), int_row, [kgrid, operators], 10**3
    )[0]
    points = join(points, send(points, lambda y, c, z, x: (y, 1 - c, z, x)))

    half = [jax.ShapeDtypeStruct((2 * depth, quarter), BF16)] * 2
    mine, theirs = call(functools.partial(cut_kernel, quarter), half, [operators], 10**3)
    blocks = [mine]
    for s in range(1, nx):
        blocks.append(send(mine, lambda y, c, z, x, s=s: gather_to(y, c, z, x, s)))
        blocks.append(
            send(theirs, lambda y, c, z, x, s=s: gather_to(y, 1 - c, z, x, s))
        )
    blocks.append(send(theirs, lambda y, c, z, x: (y, 1 - c, z, x)))

    if nz & (nz - 1):
        around = [
            send(points, lambda y, c, z, x, s=s: (y, c, (z + s) % nz, x)) for s in range(1, nz)
        ]
        points = join(points, *around)
    else:
        span = 1
        while span < nz:
            span *= 2
            other = send(points, lambda y, c, z, x, m=span - 1: (y, c, z ^ m, x))
            points = join(points, other)
    points = [points] + [
        send(points, lambda y, c, z, x, s=s: reduce_to(y, c, z, x, -s)) for s in range(1, ny)
    ]
    rows = 2 * own * nc * nz
    terms = 2 * depth * len(blocks)
    tables = call(
        functools.partial(table_kernel, sizes, order, own, depth, len(points)),
        [jax.ShapeDtypeStruct((rows, terms), BF16)] * len(points),
        [rvec, degen.reshape(1, -1)] + points,
        10**7,
    )

    if depth % SUBLANES:
        blocks = [jnp.concatenate(blocks, axis=0)]
    group = rows // nz

    def fold(chosen, coded, groups):
        shape = (group + group // 4, quarter + LANES) if coded else (group, quarter)
        kind = jax.ShapeDtypeStruct(shape, jnp.int16 if coded else F32)
        return call(
            functools.partial(fold_kernel, len(blocks), len(chosen), coded, groups[0]),
            [kind] * (len(groups) * len(chosen)),
            blocks + list(chosen),
            10**8 * len(groups),
        )

    away = []
    for groups in ([0], list(range(1, nz))):
        if not groups:
            continue
        sent = fold(tables[1:], True, groups)
        for n in groups:
            away.append(
                [
                    send(
                        sent[(s - 1) * len(groups) + n - groups[0]],
                        lambda y, c, z, x, s=s: reduce_to(y, c, z, x, s),
                    )
                    for s in range(1, ny)
                ]
            )
    kept = fold(tables[:1], False, list(range(nz)))

    bands = call(
        functools.partial(bands_kernel, own, width, lanes),
        [
            jax.ShapeDtypeStruct((own, 2 * width, 2 * lanes), BF16),
            jax.ShapeDtypeStruct((own, 2 * width, 2 * lanes), BF16),
            jax.ShapeDtypeStruct((own, 2 * lanes, 2 * lanes), BF16),
        ],
        [vectors],
        10**6,
        BANDS_SCRATCH(own, width, lanes),
    )

    rots = [None] * nz
    turns = [None] * nz
    for n, s in enumerate(order):
        both = [jax.ShapeDtypeStruct((2 * own * nc, quarter), BF16)]
        same = call(add_kernel, both, [kept[n]] + away[n], 10**5)[0]
        if s:
            same = send(same, lambda y, c, z, x, s=s: (y, c, (z + s) % nz, x))
        part = [jax.ShapeDtypeStruct((2 * own, quarter), BF16)]
        cross = call(split_kernel, part, [same], 10**3)[0]
        cross = send(cross, lambda y, c, z, x: (y, 1 - c, z, x))
        rots[s], turns[s] = call(
            functools.partial(turn_kernel, own, width, lanes),
            [
                jax.ShapeDtypeStruct((own, 2 * width, lanes), BF16),
                jax.ShapeDtypeStruct((own, width, 2 * lanes), BF16),
            ],
            [same, cross] + list(bands),
            4 * 10**8,
            TURN_SCRATCH(own, width, lanes),
        )

    density, total = call(
        functools.partial(trace_kernel, nz, own, width, lanes),
        [
            jax.ShapeDtypeStruct((3, own), F32),
            jax.ShapeDtypeStruct((count, LANES), F32),
        ],
        rots + turns,
        5 * 10**8,
        TRACE_SCRATCH(nz, own, width, lanes),
    )
    shared = lax.all_to_all(total, ALL, 0, 0, tiled=True)
    magnetization = jnp.sum(shared[:, :3], axis=0)
    return density, magnetization


def solution(mesh):
    nka, nz, nx = (mesh.shape[name] for name in ("ka", "op", "row"))
    sizes = (nka // CORES, CORES, nz, nx)
    split = Mesh(mesh.devices.reshape(sizes), ALL)
    in_specs = (
        P(None, ALL),
        P(),
        P(),
        P("op", ("y", "core", "row"), None),
        P(ALL, None),
    )
    out_specs = (P(None, ALL), P())
    return jax.shard_map(
        functools.partial(per_device, sizes),
        mesh=split,
        in_specs=in_specs,
        out_specs=out_specs,
        check_vma=False,
    )
```
